32 devices in a mesh: gx: 4 (over y, x), gy: 2 (over core), gz: 4 (over z).
Axes of the slice: x: 2, y: 2, z: 4, core: 2. Of those that a mesh axis runs over, the one named last changes fastest.
Arguments:
- flow_state: float32 [5, 128, 32, 512], P(None, 'gz', 'gy', 'gx'), may hold values from -5 to 120, as said below
- advection: float32 [3, 5], replicated, may hold values from -400 to 400, as said below
- inverse_x: float32 [5, 128, 128], replicated, may hold values from -1 to 1, as said below
- inverse_y: float32 [5, 16, 16], replicated, may hold values from -1 to 1, as said below
- inverse_z: float32 [5, 32, 32], replicated, may hold values from -1 to 1, as said below
- reduced_x: float32 [5, 16, 16], replicated, as said below
- reduced_y: float32 [5, 8, 8], replicated, as said below
- reduced_z: float32 [5, 16, 16], replicated, as said below
Outputs:
- update: float32 [5, 128, 32, 512], P(None, 'gz', 'gy', 'gx')
- rms_norm: float32 [5], replicated
The draws below stay inside these ranges and needn't reach their ends.
Inputs may be any that keep to these rules, and one draw needn't show every extreme that they name: flow_state[0] (density) lies between 0.5 and 2, and flow_state[4] / density minus half the squared velocity is at least 0.6 in every cell. `advection`: every entry has magnitude between 100 and 400. inverse_x[v] is the inverse of the 128 x 128 matrix with 4 on the diagonal, advection[0, v] / 2 - 2 just above it, -advection[0, v] / 2 - 2 just below it and 0.5 two places off it. inverse_y[v] is the inverse of the 16 x 16 matrix built likewise from advection[1, v]. inverse_z[v] is the inverse of the 32 x 32 matrix built likewise from advection[2, v]. reduced_x[v] is the inverse of I + K, K being the boundary rows and columns of the block inverses times the coupling between blocks, so that S_x equals the exact solution of the banded system along whole x lines with nothing beyond the grid's ends. reduced_y[v] is built likewise for y lines. reduced_z[v] is built likewise for z lines.
All inputs are finite; a program needn't handle non-finite values.
Results may differ from the reference program's by a relative error of at most 0.0002.
Values sent between devices are 32-bit elements.
A program may use at most 64 MiB of HBM per device.

```python
import jax
import jax.numpy as jnp
import numpy as np
from jax import lax

VARS = 5
CX = 128
CY = 16
CZ = 32
NX = 512
NY = 32
NZ = 128


fourth_coef = 0.5


def advection_table(key):
    subkeys = jax.random.split(jax.random.fold_in(key, 17), 2)
    magnitude = 100.0 * 4.0 ** jax.random.uniform(subkeys[0], (3, VARS), jnp.float32)
    signs = 2.0 * jax.random.randint(subkeys[1], (3, VARS), 0, 2).astype(jnp.float32) - 1.0
    return signs * magnitude


def band_matrix(length, speed):
    identity = jnp.eye(length, dtype=jnp.float32)
    upper_band = jnp.eye(length, k=1, dtype=jnp.float32)
    lower_band = jnp.eye(length, k=-1, dtype=jnp.float32)
    second_band = jnp.eye(length, k=2, dtype=jnp.float32) + jnp.eye(length, k=-2, dtype=jnp.float32)
    return (1.0 + 6.0 * fourth_coef) * identity + (0.5 * speed - 4.0 * fourth_coef) * upper_band + (-0.5 * speed - 4.0 * fourth_coef) * lower_band + fourth_coef * second_band


def block_inverse(key, direction, block_len):
    speeds = advection_table(key)[direction]
    return jax.vmap(lambda speed: jnp.linalg.inv(band_matrix(block_len, speed)))(speeds)


def reduced_inverse(key, direction, block_len, blocks):
    speeds = advection_table(key)[direction]
    length = block_len * blocks
    picked = (block_len * np.arange(blocks)[:, None] + np.array([0, 1, block_len - 2, block_len - 1])[None, :]).reshape(-1)

    def single(speed):
        local_block = band_matrix(block_len, speed)
        whole_line = band_matrix(length, speed)
        spread_inv = jnp.kron(jnp.eye(blocks, dtype=jnp.float32), jnp.linalg.inv(local_block))
        coupling = whole_line - jnp.kron(jnp.eye(blocks, dtype=jnp.float32), local_block)
        product = jnp.dot(spread_inv, coupling, precision=lax.Precision.HIGHEST)
        reduced_k = product[picked][:, picked]
        return jnp.linalg.inv(jnp.eye(4 * blocks, dtype=jnp.float32) + reduced_k)
    return jax.vmap(single)(speeds)


def region_envelope(key):
    phases = jax.random.uniform(jax.random.fold_in(key, 29), (2,), jnp.float32, 0.0, 6.2831853)
    along_z = jnp.arange(NZ, dtype=jnp.float32) * (6.2831853 / NZ)
    along_y = jnp.arange(NY, dtype=jnp.float32) * (6.2831853 / NY)
    shape_z = 0.5 + 0.5 * jnp.sin(along_z + phases[0])
    shape_y = 0.5 + 0.5 * jnp.cos(along_y + phases[1])
    envelope = 0.2 + 0.8 * shape_z[:, None] * shape_y[None, :]
    return envelope[:, :, None]


def draw_flow_state(key, part):
    subkeys = jax.random.split(jax.random.fold_in(key, 11), 6)
    grid_shape = (NZ, NY, NX)
    envelope = region_envelope(key)
    density = 0.5 * 4.0 ** jax.random.uniform(subkeys[0], grid_shape, jnp.float32)
    velocity = jnp.clip(0.6 * jax.random.normal(subkeys[1], (3,) + grid_shape, jnp.float32), -2.5, 2.5)
    baseline = jax.random.uniform(subkeys[2], grid_shape, jnp.float32, 0.6, 1.8)
    density = 1.0 + envelope * (density - 1.0)
    velocity = envelope[None] * velocity
    baseline = 0.6 + envelope * (baseline - 0.6)
    cell_total = NZ * NY * NX
    segment = cell_total // 8
    offsets = jax.random.randint(subkeys[3], (8,), 0, segment)
    hot_cells = jnp.arange(8, dtype=jnp.int32) * segment + offsets
    ranking = jax.random.permutation(subkeys[4], 8)
    levels = 10.0 * 1.25 ** ranking.astype(jnp.float32)
    hot_extra = jnp.zeros((cell_total,), jnp.float32).at[hot_cells].add(levels).reshape(grid_shape)
    internal = baseline + hot_extra
    momentum = density * velocity
    energy = density * (internal + 0.5 * jnp.sum(velocity * velocity, axis=0))
    return jnp.stack([density, momentum[0], momentum[1], momentum[2], energy])


def draw_advection(key, part):
    return advection_table(key)


def draw_inverse_x(key, part):
    return block_inverse(key, 0, CX)


def draw_inverse_y(key, part):
    return block_inverse(key, 1, CY)


def draw_inverse_z(key, part):
    return block_inverse(key, 2, CZ)


def draw_reduced_x(key, part):
    return reduced_inverse(key, 0, CX, NX // CX)


def draw_reduced_y(key, part):
    return reduced_inverse(key, 1, CY, NY // CY)


def draw_reduced_z(key, part):
    return reduced_inverse(key, 2, CZ, NZ // CZ)


def setup_inputs(seed: int = 0) -> dict:
    arg_keys = jax.random.split(jax.random.key(seed), 9)
    return {
        "flow_state": draw_flow_state(jax.random.fold_in(arg_keys[8], 71), 0),
        "advection": draw_advection(jax.random.fold_in(arg_keys[8], 71), 0),
        "inverse_x": draw_inverse_x(jax.random.fold_in(arg_keys[8], 71), 0),
        "inverse_y": draw_inverse_y(jax.random.fold_in(arg_keys[8], 71), 0),
        "inverse_z": draw_inverse_z(jax.random.fold_in(arg_keys[8], 71), 0),
        "reduced_x": draw_reduced_x(jax.random.fold_in(arg_keys[8], 71), 0),
        "reduced_y": draw_reduced_y(jax.random.fold_in(arg_keys[8], 71), 0),
        "reduced_z": draw_reduced_z(jax.random.fold_in(arg_keys[8], 71), 0),
    }


exact_mode = lax.Precision.HIGHEST
gas_ratio = 0.4
courant = 8000.0
damping = 0.0625
fourth_coef = 0.5

def primitives(flow_state):
    density = flow_state[0]
    velocity = flow_state[1:4] / density
    kinetic = 0.5 * lax.optimization_barrier(jnp.sum(velocity * velocity, axis=0))
    internal = jnp.maximum(flow_state[4] / density - kinetic, 0.25)
    pressure = gas_ratio * density * internal
    return (velocity, internal, pressure)

def flux_component(flow_state, velocity, pressure, variable, direction):
    carried = velocity[direction]
    if variable == 0:
        return flow_state[1 + direction]
    if variable < 4:
        moment = flow_state[variable] * carried
        if variable - 1 == direction:
            moment = moment + pressure
        return moment
    return (flow_state[4] + pressure) * carried

def residual_field(flow_state, velocity, pressure):
    collected = []
    for variable in range(VARS):
        field = flow_state[variable]
        running = jnp.zeros_like(field)
        for direction in range(3):
            line_axis = 2 - direction
            flux = flux_component(flow_state, velocity, pressure, variable, direction)
            running = running - 0.5 * (jnp.roll(flux, -1, line_axis) - jnp.roll(flux, 1, line_axis))
            fourth = jnp.roll(field, 2, line_axis) - 4.0 * jnp.roll(field, 1, line_axis) + 6.0 * field - 4.0 * jnp.roll(field, -1, line_axis) + jnp.roll(field, -2, line_axis)
            running = running - damping * fourth
        collected.append(running)
    return jnp.stack(collected)

def neighbour_table(reduced):
    blocks = reduced.shape[0] // 4
    padded = jnp.pad(reduced, ((2, 2), (0, 0)))
    picked = (4 * np.arange(blocks)[:, None] + np.array([0, 1, 6, 7])[None, :]).reshape(-1)
    return padded[picked]

def line_solve(line_field, line_axis, inverse, reduced, speed):
    moved = jnp.moveaxis(line_field, line_axis, -1)
    block_len = inverse.shape[0]
    blocks = reduced.shape[0] // 4
    leading = moved.shape[:-1]
    split = moved.reshape(leading + (blocks, block_len))
    local_part = jnp.einsum('ij,abpj->abpi', inverse, split, precision=exact_mode)
    boundary = jnp.stack([local_part[..., 0], local_part[..., 1], local_part[..., block_len - 2], local_part[..., block_len - 1]], axis=-1).reshape(leading + (4 * blocks,))
    nearby = jnp.einsum('rq,abq->abr', neighbour_table(reduced), boundary, precision=exact_mode).reshape(leading + (blocks, 4))
    lower_one = -0.5 * speed - 4.0 * fourth_coef
    upper_one = 0.5 * speed - 4.0 * fourth_coef
    left_first = fourth_coef * nearby[..., 0] + lower_one * nearby[..., 1]
    left_second = fourth_coef * nearby[..., 1]
    right_first = fourth_coef * nearby[..., 2]
    right_second = upper_one * nearby[..., 2] + fourth_coef * nearby[..., 3]
    correction = inverse[:, 0] * left_first[..., None] + inverse[:, 1] * left_second[..., None] + inverse[:, block_len - 2] * right_first[..., None] + inverse[:, block_len - 1] * right_second[..., None]
    solved = (local_part - correction).reshape(moved.shape)
    return jnp.moveaxis(solved, -1, line_axis)

def reference(flow_state, advection, inverse_x, inverse_y, inverse_z, reduced_x, reduced_y, reduced_z):
    velocity, internal, pressure = primitives(flow_state)
    wave_speed = lax.optimization_barrier(jnp.sum(jnp.abs(velocity), axis=0)) + jnp.sqrt(3.0 * 1.4 * gas_ratio * internal)
    top_speed = jnp.max(wave_speed)
    time_step = courant / top_speed
    residual = residual_field(flow_state, velocity, pressure)
    rms_norm = jnp.sqrt(lax.optimization_barrier(jnp.sum(residual * residual, axis=(1, 2, 3))) / (NX * NY * NZ))
    inverses = (inverse_x, inverse_y, inverse_z)
    reduceds = (reduced_x, reduced_y, reduced_z)
    collected = []
    for variable in range(VARS):
        line_field = time_step * residual[variable]
        for direction in range(3):
            line_field = line_solve(line_field, 2 - direction, inverses[direction][variable], reduceds[direction][variable], advection[direction, variable])
        collected.append(line_field)
    return (jnp.stack(collected), rms_norm)
```

```python
import functools

import jax
import jax.numpy as jnp
from jax import lax
from jax.experimental import pallas as pl
from jax.experimental.pallas import tpu as pltpu
from jax.sharding import PartitionSpec as P

MESH = pl.DeviceIdType.MESH
HIGHEST = lax.Precision.HIGHEST
gas_ratio = 0.4
courant = 8000.0
damping = 0.0625
fourth_coef = 0.5
AXES = ("gx", "gy", "gz")

NN = (((1,), (0,)), ((), ()))
NT = (((1,), (1,)), ((), ()))
TN = (((0,), (0,)), ((), ()))


def exact_dot(a, b, dims):
    return lax.dot_general(a, b, dims, precision=HIGHEST, preferred_element_type=jnp.float32)


def halves(a):
    high = a.astype(jnp.bfloat16)
    low = (a - high.astype(jnp.float32)).astype(jnp.bfloat16)
    return high, low


def split_dot(a, b, dims):
    def dot(x, y):
        return lax.dot_general(x, y, dims, preferred_element_type=jnp.float32)

    return dot(a[0], b[0]) + (dot(a[0], b[1]) + dot(a[1], b[0]))


def iota(shape, dim):
    return lax.broadcasted_iota(jnp.int32, shape, dim)


def primitives(u):
    inverse = 1.0 / u[0]
    velocity = [u[1] * inverse, u[2] * inverse, u[3] * inverse]
    kinetic = 0.5 * (velocity[0] * velocity[0] + velocity[1] * velocity[1] + velocity[2] * velocity[2])
    internal = jnp.maximum(u[4] * inverse - kinetic, 0.25)
    pressure = gas_ratio * u[0] * internal
    return velocity, internal, pressure


def fluxes(u, direction, values=None):
    velocity, internal, pressure = primitives(u) if values is None else values
    carried = velocity[direction]
    found = [u[1 + direction]]
    for component in range(3):
        moment = u[1 + component] * carried
        if component == direction:
            moment = moment + pressure
        found.append(moment)
    found.append((u[4] + pressure) * carried)
    return found


def coupling(reduced, index, blocks, speed, load):
    inner = jnp.where(index > 0, 1.0, 0.0).astype(jnp.float32)
    outer = jnp.where(index < blocks - 1, 1.0, 0.0).astype(jnp.float32)
    low = jnp.maximum(4 * index - 2, 0)
    high = jnp.minimum(4 * index + 4, 4 * blocks - 2)
    l0 = load(low) * inner
    l1 = load(low + 1) * inner
    f0 = load(high) * outer
    f1 = load(high + 1) * outer
    g0 = fourth_coef * l0 + (-0.5 * speed - 4.0 * fourth_coef) * l1
    g1 = fourth_coef * l1
    h0 = fourth_coef * f0
    h1 = (0.5 * speed - 4.0 * fourth_coef) * f0 + fourth_coef * f1
    return [g0, g1, h0, h1]


def kernel(dims, state, ax, ay, az, rx, sy, sz, ry, rz, adv, out, stats_out,
           uz, uy, hx, res, edge, field, first, xb, yb, zb, stx, sty, stz, khi, klo, azx,
           in_sem, halo_send, halo_recv, xs, xr, ys, yr, zs, zr, ss, sr):
    counts, nv, cz, cy, cx, cells = dims
    gx, gy, gz = counts
    rows = cz * cy
    me = [lax.axis_index(axis) for axis in AXES]

    loads = []
    for v in range(nv):
        copy = pltpu.make_async_copy(state.at[v], uz.at[v, pl.ds(2 * cy, rows)], in_sem.at[v])
        copy.start()
        loads.append(copy)

    barrier = pltpu.get_barrier_semaphore()
    total = 0
    for axis, count, place in zip(AXES, counts, me):
        for k in range(1, count):
            pl.semaphore_signal(barrier, inc=1, device_id={axis: lax.rem(place + k, count)}, device_id_type=MESH)
            total += 1
    for copy in loads:
        copy.wait()
    pl.semaphore_wait(barrier, total)

    def ring(axis, slot, down_src, down_dst, up_src, up_dst):
        count, place = counts[axis], me[axis]
        lower = lax.rem(place + count - 1, count)
        upper = lax.rem(place + 1, count)
        down = pltpu.make_async_remote_copy(
            src_ref=down_src, dst_ref=down_dst, send_sem=halo_send.at[slot], recv_sem=halo_recv.at[slot],
            device_id={AXES[axis]: lower}, device_id_type=MESH)
        up = pltpu.make_async_remote_copy(
            src_ref=up_src, dst_ref=up_dst, send_sem=halo_send.at[slot + 1], recv_sem=halo_recv.at[slot + 1],
            device_id={AXES[axis]: upper}, device_id_type=MESH)
        down.start()
        up.start()
        return [down, up]

    def spread(axis, src, dst, send, recv):
        count, place = counts[axis], me[axis]
        copies = []
        for k in range(1, count):
            copy = pltpu.make_async_remote_copy(
                src_ref=src, dst_ref=dst, send_sem=send(k - 1), recv_sem=recv(k - 1),
                device_id={AXES[axis]: lax.rem(place + k, count)}, device_id_type=MESH)
            copy.start()
            copies.append(copy)
        return copies

    z_halo = ring(2, 4,
                  uz.at[:, pl.ds(2 * cy, 2 * cy)], uz.at[:, pl.ds((cz + 2) * cy, 2 * cy)],
                  uz.at[:, pl.ds(cz * cy, 2 * cy)], uz.at[:, pl.ds(0, 2 * cy)])

    sub8, lane8 = iota((8, cx), 0), iota((8, cx), 1)
    target = jnp.where(sub8 < 2, sub8, cx - 4 + sub8)
    select = jnp.where((sub8 < 4) & (lane8 == target), 1.0, 0.0).astype(jnp.float32)
    for v in range(nv):
        hx[0, v] = exact_dot(select, uz[v, pl.ds(2 * cy, rows), :], NT)
    x_halo = ring(0, 0, hx.at[0], hx.at[1], hx.at[0], hx.at[2])

    for v in range(nv):
        for y in range(cy):
            uy[v, pl.ds((y + 2) * cz, cz), :] = uz[v, pl.ds(2 * cy + y, cz, stride=cy), :]
    y_halo = ring(1, 2,
                  uy.at[:, pl.ds(2 * cz, 2 * cz)], uy.at[:, pl.ds((cy + 2) * cz, 2 * cz)],
                  uy.at[:, pl.ds(cy * cz, 2 * cz)], uy.at[:, pl.ds(0, 2 * cz)])

    spread_z = jnp.where(iota((cz, rows), 1) // cy == iota((cz, rows), 0), 1.0, 0.0).astype(jnp.float32)
    spread_y = jnp.where(lax.rem(iota((cy, rows), 1), cy) == iota((cy, rows), 0), 1.0, 0.0).astype(jnp.float32)
    for v in range(nv):
        azx[...] = exact_dot(az[v], spread_z, NN)
        wide_y = exact_dot(ay[v], spread_y, NN)

        @pl.loop(0, cz)
        def _(z):
            high, low = halves(azx[pl.ds(z, 1), :] * wide_y)
            at = pl.ds(pl.multiple_of(z * cy, cy), cy)
            khi[v, at, :] = high
            klo[v, at, :] = low

    ux = []
    picked = iota((8 * gx, 4 * gx), 0)
    wanted = jnp.where(lax.rem(picked, 8) < 4, (picked // 8) * 4 + lax.rem(picked, 8), -1)
    expand = jnp.where(iota((8 * gx, 4 * gx), 1) == wanted, 1.0, 0.0).astype(jnp.float32)
    sub_m = iota((8, 4 * gx), 0)
    for v in range(nv):
        m = coupling(rx, me[0], gx, adv[0, v], lambda row: rx[v, pl.ds(row, 1), :])
        table = jnp.where(sub_m == 0, m[0], jnp.where(sub_m == 1, m[1], jnp.where(sub_m == 2, m[2],
                          jnp.where(sub_m == 3, m[3], 0.0))))
        columns = exact_dot(select, ax[v], NT)
        ux.append(exact_dot(exact_dot(expand, table, NT), columns, NN))

    def part(u, direction, centre_values=None):
        ahead = fluxes(u[1], direction)
        behind = fluxes(u[-1], direction)
        found = []
        for v in range(nv):
            fourth = u[-2][v] - 4.0 * u[-1][v] + 6.0 * u[0][v] - 4.0 * u[1][v] + u[2][v]
            found.append(-0.5 * (ahead[v] - behind[v]) - damping * fourth)
        return found

    for copy in y_halo:
        copy.wait_recv()

    @pl.loop(0, cy)
    def _(y):
        u = {}
        for off in range(-2, 3):
            at = pl.ds(pl.multiple_of((y + 2 + off) * cz, cz), cz)
            u[off] = [uy[v, at, :] for v in range(nv)]
        found = part(u, 1)
        for v in range(nv):
            res[v, pl.ds(y, cz, stride=cy), :] = found[v]

    for copy in x_halo:
        copy.wait_recv()
    sub_h = iota((8, rows), 0)
    merged = []
    for v in range(nv):
        fill = 1.0 if v == 0 else 0.0
        both = jnp.where(sub_h < 2, hx[1, v], hx[2, v])
        merged.append(jnp.where(sub_h < 4, both, fill))
    halo_flux = fluxes(merged, 0)

    def at_lane(row, lane, value):
        return jnp.where((sub8 == row) & (lane8 == lane), value, 0.0)

    weights = (at_lane(0, cx - 2, -damping) + at_lane(0, cx - 1, 4.0 * damping) + at_lane(1, cx - 1, -damping)
               + at_lane(2, 0, -damping) + at_lane(3, 0, 4.0 * damping) + at_lane(3, 1, -damping)
               + at_lane(4, cx - 1, -0.5) + at_lane(7, 0, 0.5)).astype(jnp.float32)
    for v in range(nv):
        stacked = jnp.where(sub_h < 4, merged[v], pltpu.roll(halo_flux[v], 4, 0))
        edge[v] = exact_dot(stacked, weights, TN)

    for copy in z_halo:
        copy.wait_recv()

    step = 2 * cy
    lane = iota((step, cx), 1)

    def shifted(a, offset):
        moved = pltpu.roll(a, (-offset) % cx, 1)
        inside = lane < cx - offset if offset > 0 else lane >= -offset
        return jnp.where(inside, moved, 0.0)

    def body(i, carry):
        squares, top = carry
        base = pl.multiple_of(i * step, step)
        u = {}
        for off in range(-2, 3):
            at = pl.ds(pl.multiple_of(base + (off + 2) * cy, cy), step)
            u[off] = [uz[v, at, :] for v in range(nv)]
        found = part(u, 2)
        values = primitives(u[0])
        velocity, internal, _ = values
        wave = (jnp.abs(velocity[0]) + jnp.abs(velocity[1]) + jnp.abs(velocity[2])
                + jnp.sqrt(3.0 * 1.4 * gas_ratio * internal))
        top = jnp.maximum(top, wave)
        flux_x = fluxes(u[0], 0, values)
        new_squares = []
        for v in range(nv):
            c = u[0][v]
            fourth = (shifted(c, -2) + shifted(c, 2)) - 4.0 * (shifted(c, -1) + shifted(c, 1)) + 6.0 * c
            along_x = -0.5 * (shifted(flux_x[v], 1) - shifted(flux_x[v], -1)) - damping * fourth
            at = pl.ds(base, step)
            value = res[v, at, :] + found[v] + (along_x + edge[v, at, :])
            res[v, at, :] = value
            new_squares.append(squares[v] + value * value)
        return tuple(new_squares), top

    zero = jnp.zeros((step, cx), jnp.float32)
    squares, top = lax.fori_loop(0, cz // 2, body, ((zero,) * nv, zero))

    x_copies = []
    for v in range(nv):
        parts = halves(res[v])
        across = halves(ax[v])
        xb[v, me[0]] = split_dot(halves(exact_dot(select, ax[v], NN)), parts, NT)
        x_copies.append(spread(0, xb.at[v, me[0]], xb.at[v, me[0]],
                               lambda k: xs.at[v, k], lambda k: xr.at[v, k]))
        first[v] = split_dot(parts, across, NT)

    sub_s = iota((8, cx), 0)
    tile = jnp.where(sub_s == 5, jnp.max(top, axis=0, keepdims=True), 0.0)
    for v in range(nv):
        tile = jnp.where(sub_s == v, jnp.sum(squares[v], axis=0, keepdims=True), tile)
    stx[me[0]] = tile
    stat_copies = [spread(0, stx.at[me[0]], stx.at[me[0]], lambda k: ss.at[0, k], lambda k: sr.at[0, k])]

    def gathered(ref, count):
        result = ref[0]
        for q in range(1, count):
            result = jnp.where(sub_s < nv, result + ref[q], jnp.maximum(result, ref[q]))
        return result

    y_copies = []
    marks_y = (0, 1, cy - 2, cy - 1)
    marks_z = (0, 1, cz - 2, cz - 1)
    for v in range(nv):
        for copy in x_copies[v]:
            copy.wait_recv()
        every = xb[v].reshape(8 * gx, rows)
        solved = first[v] - split_dot(halves(every), halves(ux[v]), TN)
        parts = halves(solved)
        field[v] = split_dot((khi[v], klo[v]), parts, NN)
        for c, mark in enumerate(marks_y):
            yb[v, me[1], pl.ds(c * cz, cz), :] = field[v, pl.ds(mark, cz, stride=cy), :]
        y_copies.append(spread(1, yb.at[v, me[1]], yb.at[v, me[1]],
                               lambda k: ys.at[v, k], lambda k: yr.at[v, k]))

    for copy in stat_copies[0]:
        copy.wait_recv()
    sty[me[1]] = gathered(stx, gx)
    stat_copies.append(spread(1, sty.at[me[1]], sty.at[me[1]], lambda k: ss.at[1, k], lambda k: sr.at[1, k]))

    def combined(reduced, inverse, axis, v, direction, planes, size):
        count = counts[axis]
        sums = [None] * 4
        for j in range(4 * count):
            m = coupling(reduced, me[axis], count, adv[direction, v], lambda row: reduced[v, row, j])
            plane = planes[v, j // 4, pl.ds((j % 4) * size, size), :]
            for c in range(4):
                term = m[c] * plane
                sums[c] = term if sums[c] is None else sums[c] + term
        return sums

    z_copies = []
    for v in range(nv):
        for copy in y_copies[v]:
            copy.wait_recv()
        sums = combined(ry, sy, 1, v, 1, yb, cz)
        for y in range(cy):
            at = pl.ds(y, cz, stride=cy)
            value = field[v, at, :]
            for c, mark in enumerate(marks_y):
                value = value - sy[v, y, mark] * sums[c]
            field[v, at, :] = value
        zb[v, me[2], pl.ds(0, 2 * cy), :] = field[v, pl.ds(0, 2 * cy), :]
        zb[v, me[2], pl.ds(2 * cy, 2 * cy), :] = field[v, pl.ds((cz - 2) * cy, 2 * cy), :]
        z_copies.append(spread(2, zb.at[v, me[2]], zb.at[v, me[2]],
                               lambda k: zs.at[v, k], lambda k: zr.at[v, k]))
        if v == 0:
            for copy in stat_copies[1]:
                copy.wait_recv()
            stz[me[2]] = gathered(sty, gy)
            stat_copies.append(spread(2, stz.at[me[2]], stz.at[me[2]],
                                      lambda k: ss.at[2, k], lambda k: sr.at[2, k]))

    for copy in stat_copies[2]:
        copy.wait_recv()
    final = gathered(stz, gz)
    norm = jnp.sqrt(jnp.sum(final, axis=1, keepdims=True) / float(cells))
    fastest = courant / jnp.max(final, axis=1, keepdims=True)
    stats_out[...] = jnp.where(sub_s < nv, norm, fastest)
    for v in range(nv):
        for copy in z_copies[v]:
            copy.wait_recv()
        sums = combined(rz, sz, 2, v, 2, zb, cy)
        for z in range(cz):
            value = field[v, pl.ds(z * cy, cy), :]
            for c, mark in enumerate(marks_z):
                value = value - sz[v, z, mark] * sums[c]
            out[v, pl.ds(z * cy, cy), :] = value

    for group in [x_halo, y_halo, z_halo] + x_copies + y_copies + z_copies + stat_copies:
        for copy in group:
            copy.wait_send()


def shards(counts, flow_state, advection, inverse_x, inverse_y, inverse_z, reduced_x, reduced_y, reduced_z):
    nv, cz, cy, cx = flow_state.shape
    gx, gy, gz = counts
    rows = cz * cy
    cells = rows * cx * gx * gy * gz
    most = max(counts) - 1
    vmem = pl.BlockSpec(memory_space=pltpu.VMEM)
    smem = pl.BlockSpec(memory_space=pltpu.SMEM)
    f32 = jnp.float32
    dma = pltpu.SemaphoreType.DMA
    out, stats = pl.pallas_call(
        functools.partial(kernel, (counts, nv, cz, cy, cx, cells)),
        out_shape=(jax.ShapeDtypeStruct((nv, rows, cx), f32), jax.ShapeDtypeStruct((8, cx), f32)),
        in_specs=[pl.BlockSpec(memory_space=pl.ANY), vmem, vmem, vmem, vmem, smem, smem, smem, smem, smem],
        out_specs=(vmem, vmem),
        scratch_shapes=[
            pltpu.VMEM((nv, (cz + 4) * cy, cx), f32),
            pltpu.VMEM((nv, (cy + 4) * cz, cx), f32),
            pltpu.VMEM((3, nv, 8, rows), f32),
            pltpu.VMEM((nv, rows, cx), f32),
            pltpu.VMEM((nv, rows, cx), f32),
            pltpu.VMEM((nv, rows, cx), f32),
            pltpu.VMEM((nv, rows, cx), f32),
            pltpu.VMEM((nv, gx, 8, rows), f32),
            pltpu.VMEM((nv, gy, 4 * cz, cx), f32),
            pltpu.VMEM((nv, gz, 4 * cy, cx), f32),
            pltpu.VMEM((gx, 8, cx), f32),
            pltpu.VMEM((gy, 8, cx), f32),
            pltpu.VMEM((gz, 8, cx), f32),
            pltpu.VMEM((nv, rows, rows), jnp.bfloat16),
            pltpu.VMEM((nv, rows, rows), jnp.bfloat16),
            pltpu.VMEM((cz, rows), f32),
            dma((nv,)),
            dma((6,)), dma((6,)),
            dma((nv, gx - 1)), dma((nv, gx - 1)),
            dma((nv, gy - 1)), dma((nv, gy - 1)),
            dma((nv, gz - 1)), dma((nv, gz - 1)),
            dma((3, most)), dma((3, most)),
        ],
        compiler_params=pltpu.CompilerParams(
            collective_id=0, has_side_effects=True, vmem_limit_bytes=60 * 1024 * 1024),
    )(flow_state.reshape(nv, rows, cx), inverse_x, inverse_y, inverse_z, reduced_x, inverse_y, inverse_z,
      reduced_y, reduced_z, advection)
    update = (out * stats[5, 0]).reshape(flow_state.shape)
    return update, stats[:nv, 0]


def solution(mesh):
    counts = tuple(mesh.shape[axis] for axis in AXES)
    placed = (P(None, "gz", "gy", "gx"), P(), P(), P(), P(), P(), P(), P())
    return jax.shard_map(
        functools.partial(shards, counts),
        mesh=mesh,
        in_specs=placed,
        out_specs=(P(None, "gz", "gy", "gx"), P()),
        check_vma=False,
    )
```

```python
import functools

import jax
import jax.numpy as jnp
from jax import lax
from jax.experimental import pallas as pl
from jax.experimental.pallas import tpu as pltpu
from jax.sharding import PartitionSpec as P

MESH = pl.DeviceIdType.MESH
HIGHEST = lax.Precision.HIGHEST
gas_ratio = 0.4
courant = 8000.0
damping = 0.0625
fourth_coef = 0.5
AXES = ("gx", "gy", "gz")

NN = (((1,), (0,)), ((), ()))
NT = (((1,), (1,)), ((), ()))
TN = (((0,), (0,)), ((), ()))


def exact_dot(a, b, dims):
    return lax.dot_general(a, b, dims, precision=HIGHEST, preferred_element_type=jnp.float32)


def halves(a):
    high = a.astype(jnp.bfloat16)
    low = (a - high.astype(jnp.float32)).astype(jnp.bfloat16)
    return high, low


def split_dot(a, b, dims):
    def dot(x, y):
        return lax.dot_general(x, y, dims, preferred_element_type=jnp.float32)

    return dot(a[0], b[0]) + (dot(a[0], b[1]) + dot(a[1], b[0]))


def iota(shape, dim):
    return lax.broadcasted_iota(jnp.int32, shape, dim)


def primitives(u):
    inverse = 1.0 / u[0]
    velocity = [u[1] * inverse, u[2] * inverse, u[3] * inverse]
    kinetic = 0.5 * (velocity[0] * velocity[0] + velocity[1] * velocity[1] + velocity[2] * velocity[2])
    internal = jnp.maximum(u[4] * inverse - kinetic, 0.25)
    pressure = gas_ratio * u[0] * internal
    return velocity, internal, pressure


def fluxes(u, direction, values=None):
    velocity, internal, pressure = primitives(u) if values is None else values
    carried = velocity[direction]
    found = [u[1 + direction]]
    for component in range(3):
        moment = u[1 + component] * carried
        if component == direction:
            moment = moment + pressure
        found.append(moment)
    found.append((u[4] + pressure) * carried)
    return found


def coupling(reduced, index, blocks, speed, load):
    inner = jnp.where(index > 0, 1.0, 0.0).astype(jnp.float32)
    outer = jnp.where(index < blocks - 1, 1.0, 0.0).astype(jnp.float32)
    low = jnp.maximum(4 * index - 2, 0)
    high = jnp.minimum(4 * index + 4, 4 * blocks - 2)
    l0 = load(low) * inner
    l1 = load(low + 1) * inner
    f0 = load(high) * outer
    f1 = load(high + 1) * outer
    g0 = fourth_coef * l0 + (-0.5 * speed - 4.0 * fourth_coef) * l1
    g1 = fourth_coef * l1
    h0 = fourth_coef * f0
    h1 = (0.5 * speed - 4.0 * fourth_coef) * f0 + fourth_coef * f1
    return [g0, g1, h0, h1]


def kernel(dims, state, ax_in, ay_in, az_in, rx_in, ry_in, rz_in, adv, out, rms_out,
           ax, ay, az, rx, sy, sz, ry, rz,
           uz, uy, hx, res, edge, field, first, xb, yb, zt, stx, sty, stz, khi, klo, azx,
           in_sem, table_sem, halo_send, halo_recv, xs, xr, ys, yr, zs, zr, ss, sr):
    counts, nv, cz, cy, cx, cells = dims
    gx, gy, gz = counts
    rows = cz * cy
    me = [lax.axis_index(axis) for axis in AXES]

    loads = []
    for v in range(nv):
        copy = pltpu.make_async_copy(state.at[v], uz.at[v, pl.ds(2 * cy, rows)], in_sem.at[v])
        copy.start()
        loads.append(copy)
    tables = []
    for slot, (source, target) in enumerate(((ax_in, ax), (ay_in, ay), (az_in, az), (rx_in, rx),
                                             (ry_in, ry), (rz_in, rz), (ay_in, sy), (az_in, sz))):
        copy = pltpu.make_async_copy(source, target, table_sem.at[slot])
        copy.start()
        tables.append(copy)

    barrier = pltpu.get_barrier_semaphore()
    total = 0
    for axis, count, place in zip(AXES, counts, me):
        for k in range(1, count):
            pl.semaphore_signal(barrier, inc=1, device_id={axis: lax.rem(place + k, count)}, device_id_type=MESH)
            total += 1
    for copy in loads:
        copy.wait()
    pl.semaphore_wait(barrier, total)

    def ring(axis, slot, down_src, down_dst, up_src, up_dst):
        count, place = counts[axis], me[axis]
        lower = lax.rem(place + count - 1, count)
        upper = lax.rem(place + 1, count)
        down = pltpu.make_async_remote_copy(
            src_ref=down_src, dst_ref=down_dst, send_sem=halo_send.at[slot], recv_sem=halo_recv.at[slot],
            device_id={AXES[axis]: lower}, device_id_type=MESH)
        up = pltpu.make_async_remote_copy(
            src_ref=up_src, dst_ref=up_dst, send_sem=halo_send.at[slot + 1], recv_sem=halo_recv.at[slot + 1],
            device_id={AXES[axis]: upper}, device_id_type=MESH)
        down.start()
        up.start()
        return [down, up]

    def spread(axis, src, dst, send, recv):
        count, place = counts[axis], me[axis]
        copies = []
        for k in range(1, count):
            copy = pltpu.make_async_remote_copy(
                src_ref=src, dst_ref=dst, send_sem=send(k - 1), recv_sem=recv(k - 1),
                device_id={AXES[axis]: lax.rem(place + k, count)}, device_id_type=MESH)
            copy.start()
            copies.append(copy)
        return copies

    z_halo = ring(2, 4,
                  uz.at[:, pl.ds(2 * cy, 2 * cy)], uz.at[:, pl.ds((cz + 2) * cy, 2 * cy)],
                  uz.at[:, pl.ds(cz * cy, 2 * cy)], uz.at[:, pl.ds(0, 2 * cy)])

    sub8, lane8 = iota((8, cx), 0), iota((8, cx), 1)
    target = jnp.where(sub8 < 2, sub8, cx - 4 + sub8)
    select = jnp.where((sub8 < 4) & (lane8 == target), 1.0, 0.0).astype(jnp.float32)
    sub_h = iota((8, rows), 0)
    for group in range(0, nv, 4):
        low = jnp.zeros((8, rows), jnp.float32)
        high = low
        for v in range(group, min(group + 4, nv)):
            place = v - group
            ends = exact_dot(select, uz[v, pl.ds(2 * cy, rows), :], NT)
            mine = sub_h // 2 == place
            low = jnp.where(mine, pltpu.roll(ends, (2 * place) % 8, 0), low)
            high = jnp.where(mine, pltpu.roll(ends, (2 * place - 2) % 8, 0), high)
        hx[0, group // 4] = low
        hx[1, group // 4] = high
    x_halo = ring(0, 0, hx.at[0], hx.at[2], hx.at[1], hx.at[3])

    for v in range(nv):
        for y in range(cy):
            uy[v, pl.ds((y + 2) * cz, cz), :] = uz[v, pl.ds(2 * cy + y, cz, stride=cy), :]
    y_halo = ring(1, 2,
                  uy.at[:, pl.ds(2 * cz, 2 * cz)], uy.at[:, pl.ds((cy + 2) * cz, 2 * cz)],
                  uy.at[:, pl.ds(cy * cz, 2 * cz)], uy.at[:, pl.ds(0, 2 * cz)])

    for copy in tables[:4]:
        copy.wait()

    spread_z = jnp.where(iota((cz, rows), 1) // cy == iota((cz, rows), 0), 1.0, 0.0).astype(jnp.float32)
    spread_y = jnp.where(lax.rem(iota((cy, rows), 1), cy) == iota((cy, rows), 0), 1.0, 0.0).astype(jnp.float32)
    for v in range(nv):
        azx[...] = exact_dot(az[v], spread_z, NN)
        wide_y = exact_dot(ay[v], spread_y, NN)

        @pl.loop(0, cz)
        def _(z):
            high, low = halves(azx[pl.ds(z, 1), :] * wide_y)
            at = pl.ds(pl.multiple_of(z * cy, cy), cy)
            khi[v, at, :] = high
            klo[v, at, :] = low

    ux = []
    picked = iota((8 * gx, 4 * gx), 0)
    wanted = jnp.where(lax.rem(picked, 8) < 4, (picked // 8) * 4 + lax.rem(picked, 8), -1)
    expand = jnp.where(iota((8 * gx, 4 * gx), 1) == wanted, 1.0, 0.0).astype(jnp.float32)
    sub_m = iota((8, 4 * gx), 0)
    for v in range(nv):
        m = coupling(rx, me[0], gx, adv[0, v], lambda row: rx[v, pl.ds(row, 1), :])
        table = jnp.where(sub_m == 0, m[0], jnp.where(sub_m == 1, m[1], jnp.where(sub_m == 2, m[2],
                          jnp.where(sub_m == 3, m[3], 0.0))))
        columns = exact_dot(select, ax[v], NT)
        ux.append(exact_dot(exact_dot(expand, table, NT), columns, NN))

    def part(u, direction, centre_values=None):
        ahead = fluxes(u[1], direction)
        behind = fluxes(u[-1], direction)
        found = []
        for v in range(nv):
            fourth = u[-2][v] - 4.0 * u[-1][v] + 6.0 * u[0][v] - 4.0 * u[1][v] + u[2][v]
            found.append(-0.5 * (ahead[v] - behind[v]) - damping * fourth)
        return found

    for copy in y_halo:
        copy.wait_recv()

    @pl.loop(0, cy)
    def _(y):
        u = {}
        for off in range(-2, 3):
            at = pl.ds(pl.multiple_of((y + 2 + off) * cz, cz), cz)
            u[off] = [uy[v, at, :] for v in range(nv)]
        found = part(u, 1)
        for v in range(nv):
            res[v, pl.ds(y, cz, stride=cy), :] = found[v]

    for copy in x_halo:
        copy.wait_recv()
    merged = []
    for v in range(nv):
        fill = 1.0 if v == 0 else 0.0
        place = v % 4
        both = jnp.where(sub_h < 2, pltpu.roll(hx[2, v // 4], (-2 * place) % 8, 0),
                         pltpu.roll(hx[3, v // 4], (2 - 2 * place) % 8, 0))
        merged.append(jnp.where(sub_h < 4, both, fill))
    halo_flux = fluxes(merged, 0)

    def at_lane(row, lane, value):
        return jnp.where((sub8 == row) & (lane8 == lane), value, 0.0)

    weights = (at_lane(0, cx - 2, -damping) + at_lane(0, cx - 1, 4.0 * damping) + at_lane(1, cx - 1, -damping)
               + at_lane(2, 0, -damping) + at_lane(3, 0, 4.0 * damping) + at_lane(3, 1, -damping)
               + at_lane(4, cx - 1, -0.5) + at_lane(7, 0, 0.5)).astype(jnp.float32)
    for v in range(nv):
        stacked = jnp.where(sub_h < 4, merged[v], pltpu.roll(halo_flux[v], 4, 0))
        edge[v] = exact_dot(stacked, weights, TN)

    for copy in z_halo:
        copy.wait_recv()

    step = 2 * cy
    lane = iota((step, cx), 1)

    def shifted(a, offset):
        moved = pltpu.roll(a, (-offset) % cx, 1)
        inside = lane < cx - offset if offset > 0 else lane >= -offset
        return jnp.where(inside, moved, 0.0)

    def body(i, carry):
        squares, top = carry
        base = pl.multiple_of(i * step, step)
        u = {}
        for off in range(-2, 3):
            at = pl.ds(pl.multiple_of(base + (off + 2) * cy, cy), step)
            u[off] = [uz[v, at, :] for v in range(nv)]
        found = part(u, 2)
        values = primitives(u[0])
        velocity, internal, _ = values
        wave = (jnp.abs(velocity[0]) + jnp.abs(velocity[1]) + jnp.abs(velocity[2])
                + jnp.sqrt(3.0 * 1.4 * gas_ratio * internal))
        top = jnp.maximum(top, wave)
        flux_x = fluxes(u[0], 0, values)
        new_squares = []
        for v in range(nv):
            c = u[0][v]
            fourth = (shifted(c, -2) + shifted(c, 2)) - 4.0 * (shifted(c, -1) + shifted(c, 1)) + 6.0 * c
            along_x = -0.5 * (shifted(flux_x[v], 1) - shifted(flux_x[v], -1)) - damping * fourth
            at = pl.ds(base, step)
            value = res[v, at, :] + found[v] + (along_x + edge[v, at, :])
            res[v, at, :] = value
            new_squares.append(squares[v] + value * value)
        return tuple(new_squares), top

    zero = jnp.zeros((step, cx), jnp.float32)
    squares, top = lax.fori_loop(0, cz // 2, body, ((zero,) * nv, zero))

    x_copies = []
    for v in range(nv):
        parts = halves(res[v])
        across = halves(ax[v])
        xb[v, me[0]] = split_dot(halves(exact_dot(select, ax[v], NN)), parts, NT)
        x_copies.append(spread(0, xb.at[v, me[0]], xb.at[v, me[0]],
                               lambda k: xs.at[v, k], lambda k: xr.at[v, k]))
        first[v] = split_dot(parts, across, NT)

    sub_s = iota((8, cx), 0)
    tile = jnp.where(sub_s == 5, jnp.max(top, axis=0, keepdims=True), 0.0)
    for v in range(nv):
        tile = jnp.where(sub_s == v, jnp.sum(squares[v], axis=0, keepdims=True), tile)
    stx[me[0]] = tile
    stat_copies = [spread(0, stx.at[me[0]], stx.at[me[0]], lambda k: ss.at[0, k], lambda k: sr.at[0, k])]

    def gathered(ref, count):
        result = ref[0]
        for q in range(1, count):
            result = jnp.where(sub_s < nv, result + ref[q], jnp.maximum(result, ref[q]))
        return result

    y_copies = []
    marks_y = (0, 1, cy - 2, cy - 1)
    marks_z = (0, 1, cz - 2, cz - 1)
    for v in range(nv):
        for copy in x_copies[v]:
            copy.wait_recv()
        every = xb[v].reshape(8 * gx, rows)
        solved = first[v] - split_dot(halves(every), halves(ux[v]), TN)
        parts = halves(solved)
        field[v] = split_dot((khi[v], klo[v]), parts, NN)
        for c, mark in enumerate(marks_y):
            yb[v, me[1], pl.ds(c * cz, cz), :] = field[v, pl.ds(mark, cz, stride=cy), :]
        y_copies.append(spread(1, yb.at[v, me[1]], yb.at[v, me[1]],
                               lambda k: ys.at[v, k], lambda k: yr.at[v, k]))

    for copy in stat_copies[0]:
        copy.wait_recv()
    sty[me[1]] = gathered(stx, gx)
    stat_copies.append(spread(1, sty.at[me[1]], sty.at[me[1]], lambda k: ss.at[1, k], lambda k: sr.at[1, k]))

    def combined(reduced, inverse, axis, v, direction, planes, size):
        count = counts[axis]
        sums = [None] * 4
        for j in range(4 * count):
            m = coupling(reduced, me[axis], count, adv[direction, v], lambda row: reduced[v, row, j])
            plane = planes[v, j // 4, pl.ds((j % 4) * size, size), :]
            for c in range(4):
                term = m[c] * plane
                sums[c] = term if sums[c] is None else sums[c] + term
        return sums

    level, levels = me[2], gz
    low = jnp.maximum(4 * level - 2, 0)
    high = jnp.minimum(4 * level + 4, 4 * levels - 2)
    own = 4 * level
    has_low, has_high = level > 0, level < levels - 1
    z_copies = []
    for v in range(nv):
        up = pltpu.make_async_remote_copy(
            src_ref=zt.at[v, 0], dst_ref=zt.at[v, 2], send_sem=zs.at[v, 0], recv_sem=zr.at[v, 0],
            device_id={"gz": jnp.minimum(level + 1, levels - 1)}, device_id_type=MESH)
        down = pltpu.make_async_remote_copy(
            src_ref=zt.at[v, 1], dst_ref=zt.at[v, 3], send_sem=zs.at[v, 1], recv_sem=zr.at[v, 1],
            device_id={"gz": jnp.maximum(level - 1, 0)}, device_id_type=MESH)
        z_copies.append((up, down))

    def planes_of(v):
        return [field[v, pl.ds(mark * cy, cy), :] for mark in marks_z]

    def from_own(v, row, planes):
        return ((rz[v, row, own] * planes[0] + rz[v, row, own + 1] * planes[1])
                + (rz[v, row, own + 2] * planes[2] + rz[v, row, own + 3] * planes[3]))

    def carrier(v, corner, valid):
        x00, x01 = rz[v, corner, corner], rz[v, corner, corner + 1]
        x10, x11 = rz[v, corner + 1, corner], rz[v, corner + 1, corner + 1]
        inverse = 1.0 / jnp.full((cy, cx), jnp.where(valid, x00 * x11 - x01 * x10, 1.0), jnp.float32)

        def apply(row, pair):
            a, b = rz[v, row, corner], rz[v, row, corner + 1]
            return ((a * x11 - b * x10) * pair[0] + (b * x00 - a * x01) * pair[1]) * inverse

        return apply

    def pair_of(v, slot):
        return [zt[v, slot, pl.ds(0, cy), :], zt[v, slot, pl.ds(cy, cy), :]]

    for copy in tables[4:]:
        copy.wait()
    for v in range(nv):
        for copy in y_copies[v]:
            copy.wait_recv()
        sums = combined(ry, sy, 1, v, 1, yb, cz)
        for y in range(cy):
            at = pl.ds(y, cz, stride=cy)
            value = field[v, at, :]
            for c, mark in enumerate(marks_y):
                value = value - sy[v, y, mark] * sums[c]
            field[v, at, :] = value
        planes = planes_of(v)
        for r in range(2):
            zt[v, 0, pl.ds(r * cy, cy), :] = from_own(v, own + 2 + r, planes)
            zt[v, 1, pl.ds(r * cy, cy), :] = from_own(v, own + r, planes)

        @pl.when(level == 0)
        def _():
            zt[v, 2] = jnp.zeros((2 * cy, cx), jnp.float32)
            z_copies[v][0].start()

        @pl.when(level == levels - 1)
        def _():
            zt[v, 3] = jnp.zeros((2 * cy, cx), jnp.float32)
            z_copies[v][1].start()

        if v == 0:
            for copy in stat_copies[1]:
                copy.wait_recv()
            stz[me[2]] = gathered(sty, gy)
            stat_copies.append(spread(2, stz.at[me[2]], stz.at[me[2]],
                                      lambda k: ss.at[2, k], lambda k: sr.at[2, k]))

    for v in range(nv):
        up, down = z_copies[v]

        @pl.when(has_low)
        def _():
            up.wait_recv()

        @pl.when(has_low & has_high)
        def _():
            pair, apply = pair_of(v, 2), carrier(v, low, has_low)
            for r in range(2):
                at = pl.ds(r * cy, cy)
                zt[v, 0, at, :] = zt[v, 0, at, :] + apply(own + 2 + r, pair)
            up.start()

        @pl.when(has_high)
        def _():
            down.wait_recv()

        @pl.when(has_low & has_high)
        def _():
            pair, apply = pair_of(v, 3), carrier(v, high, has_high)
            for r in range(2):
                at = pl.ds(r * cy, cy)
                zt[v, 1, at, :] = zt[v, 1, at, :] + apply(own + r, pair)
            down.start()

    for copy in stat_copies[2]:
        copy.wait_recv()
    final = gathered(stz, gz)
    norm = jnp.sqrt(jnp.sum(final, axis=1, keepdims=True) / float(cells))
    norm = jnp.broadcast_to(norm, (8, cx))
    for v in range(nv):
        rms_out[v] = norm[v, 0]
    fastest = jnp.broadcast_to(courant / jnp.max(final, axis=1, keepdims=True), (8, cx))
    time_step = jnp.broadcast_to(fastest[5:6, :], (cy, cx))
    inner = jnp.where(has_low, 1.0, 0.0).astype(jnp.float32)
    outer = jnp.where(has_high, 1.0, 0.0).astype(jnp.float32)
    for v in range(nv):
        planes = planes_of(v)
        below, above = pair_of(v, 2), pair_of(v, 3)
        lift, sink = carrier(v, low, has_low), carrier(v, high, has_high)
        l = [inner * (below[r] + from_own(v, low + r, planes) + sink(low + r, above)) for r in range(2)]
        f = [outer * (above[r] + from_own(v, high + r, planes) + lift(high + r, below)) for r in range(2)]
        speed = adv[2, v]
        sums = [fourth_coef * l[0] + (-0.5 * speed - 4.0 * fourth_coef) * l[1],
                fourth_coef * l[1],
                fourth_coef * f[0],
                (0.5 * speed - 4.0 * fourth_coef) * f[0] + fourth_coef * f[1]]
        for z in range(cz):
            value = field[v, pl.ds(z * cy, cy), :]
            for c, mark in enumerate(marks_z):
                value = value - sz[v, z, mark] * sums[c]
            out[v, pl.ds(z * cy, cy), :] = value * time_step

    for group in [x_halo, y_halo, z_halo] + x_copies + y_copies + stat_copies:
        for copy in group:
            copy.wait_send()
    for v in range(nv):
        @pl.when(has_high)
        def _():
            z_copies[v][0].wait_send()

        @pl.when(has_low)
        def _():
            z_copies[v][1].wait_send()


def shards(counts, flow_state, advection, inverse_x, inverse_y, inverse_z, reduced_x, reduced_y, reduced_z):
    nv, cz, cy, cx = flow_state.shape
    gx, gy, gz = counts
    rows = cz * cy
    cells = rows * cx * gx * gy * gz
    most = max(counts) - 1
    vmem = pl.BlockSpec(memory_space=pltpu.VMEM)
    smem = pl.BlockSpec(memory_space=pltpu.SMEM)
    f32 = jnp.float32
    dma = pltpu.SemaphoreType.DMA
    hbm = pl.BlockSpec(memory_space=pl.ANY)
    out, rms = pl.pallas_call(
        functools.partial(kernel, (counts, nv, cz, cy, cx, cells)),
        out_shape=(jax.ShapeDtypeStruct((nv, rows, cx), f32), jax.ShapeDtypeStruct((nv,), f32)),
        in_specs=[hbm] * 7 + [smem],
        out_specs=(vmem, smem),
        scratch_shapes=[
            pltpu.VMEM(inverse_x.shape, f32),
            pltpu.VMEM(inverse_y.shape, f32),
            pltpu.VMEM(inverse_z.shape, f32),
            pltpu.VMEM(reduced_x.shape, f32),
            pltpu.SMEM(inverse_y.shape, f32),
            pltpu.SMEM(inverse_z.shape, f32),
            pltpu.SMEM(reduced_y.shape, f32),
            pltpu.SMEM(reduced_z.shape, f32),
            pltpu.VMEM((nv, (cz + 4) * cy, cx), f32),
            pltpu.VMEM((nv, (cy + 4) * cz, cx), f32),
            pltpu.VMEM((4, -(-nv // 4), 8, rows), f32),
            pltpu.VMEM((nv, rows, cx), f32),
            pltpu.VMEM((nv, rows, cx), f32),
            pltpu.VMEM((nv, rows, cx), f32),
            pltpu.VMEM((nv, rows, cx), f32),
            pltpu.VMEM((nv, gx, 8, rows), f32),
            pltpu.VMEM((nv, gy, 4 * cz, cx), f32),
            pltpu.VMEM((nv, 4, 2 * cy, cx), f32),
            pltpu.VMEM((gx, 8, cx), f32),
            pltpu.VMEM((gy, 8, cx), f32),
            pltpu.VMEM((gz, 8, cx), f32),
            pltpu.VMEM((nv, rows, rows), jnp.bfloat16),
            pltpu.VMEM((nv, rows, rows), jnp.bfloat16),
            pltpu.VMEM((cz, rows), f32),
            dma((nv,)), dma((8,)),
            dma((6,)), dma((6,)),
            dma((nv, gx - 1)), dma((nv, gx - 1)),
            dma((nv, gy - 1)), dma((nv, gy - 1)),
            dma((nv, 2)), dma((nv, 2)),
            dma((3, most)), dma((3, most)),
        ],
        compiler_params=pltpu.CompilerParams(
            collective_id=0, has_side_effects=True, vmem_limit_bytes=60 * 1024 * 1024),
    )(flow_state.reshape(nv, rows, cx), inverse_x, inverse_y, inverse_z, reduced_x, reduced_y, reduced_z,
      advection)
    return out.reshape(flow_state.shape), rms


def solution(mesh):
    counts = tuple(mesh.shape[axis] for axis in AXES)
    placed = (P(None, "gz", "gy", "gx"), P(), P(), P(), P(), P(), P(), P())
    return jax.shard_map(
        functools.partial(shards, counts),
        mesh=mesh,
        in_specs=placed,
        out_specs=(P(None, "gz", "gy", "gx"), P()),
        check_vma=False,
    )
```

```python
import functools

import jax
import jax.numpy as jnp
from jax import lax
from jax.experimental import pallas as pl
from jax.experimental.pallas import tpu as pltpu
from jax.sharding import PartitionSpec as P

MESH = pl.DeviceIdType.MESH
HIGHEST = lax.Precision.HIGHEST
gas_ratio = 0.4
courant = 8000.0
damping = 0.0625
fourth_coef = 0.5
AXES = ("gx", "gy", "gz")

NN = (((1,), (0,)), ((), ()))
NT = (((1,), (1,)), ((), ()))
TN = (((0,), (0,)), ((), ()))


def exact_dot(a, b, dims):
    return lax.dot_general(a, b, dims, precision=HIGHEST, preferred_element_type=jnp.float32)


def halves(a):
    high = a.astype(jnp.bfloat16)
    low = (a - high.astype(jnp.float32)).astype(jnp.bfloat16)
    return high, low


def split_dot(a, b, dims):
    def dot(x, y):
        return lax.dot_general(x, y, dims, preferred_element_type=jnp.float32)

    return dot(a[0], b[0]) + (dot(a[0], b[1]) + dot(a[1], b[0]))


def iota(shape, dim):
    return lax.broadcasted_iota(jnp.int32, shape, dim)


def primitives(u):
    inverse = 1.0 / u[0]
    velocity = [u[1] * inverse, u[2] * inverse, u[3] * inverse]
    kinetic = 0.5 * (velocity[0] * velocity[0] + velocity[1] * velocity[1] + velocity[2] * velocity[2])
    internal = jnp.maximum(u[4] * inverse - kinetic, 0.25)
    pressure = gas_ratio * u[0] * internal
    return velocity, internal, pressure


def fluxes(u, direction, values=None):
    velocity, internal, pressure = primitives(u) if values is None else values
    carried = velocity[direction]
    found = [u[1 + direction]]
    for component in range(3):
        moment = u[1 + component] * carried
        if component == direction:
            moment = moment + pressure
        found.append(moment)
    found.append((u[4] + pressure) * carried)
    return found


def coupling(reduced, index, blocks, speed, load):
    inner = jnp.where(index > 0, 1.0, 0.0).astype(jnp.float32)
    outer = jnp.where(index < blocks - 1, 1.0, 0.0).astype(jnp.float32)
    low = jnp.maximum(4 * index - 2, 0)
    high = jnp.minimum(4 * index + 4, 4 * blocks - 2)
    l0 = load(low) * inner
    l1 = load(low + 1) * inner
    f0 = load(high) * outer
    f1 = load(high + 1) * outer
    g0 = fourth_coef * l0 + (-0.5 * speed - 4.0 * fourth_coef) * l1
    g1 = fourth_coef * l1
    h0 = fourth_coef * f0
    h1 = (0.5 * speed - 4.0 * fourth_coef) * f0 + fourth_coef * f1
    return [g0, g1, h0, h1]


def kernel(dims, state, ax_in, ay_in, az_in, rx_in, ry_in, rz_in, adv, out, rms_out,
           ax, ay, az, rx, sy, sz, ry, rz,
           uz, uy, hx, res, edge, field, first, xb, yb, zt, stx, sty, stz, khi, klo, azx,
           in_sem, table_sem, halo_send, halo_recv, xs, xr, ys, yr, zs, zr, ss, sr):
    counts, nv, cz, cy, cx, cells = dims
    gx, gy, gz = counts
    rows = cz * cy
    me = [lax.axis_index(axis) for axis in AXES]

    loads = []
    for v in range(nv):
        copy = pltpu.make_async_copy(state.at[v], uz.at[v, pl.ds(2 * cy, rows)], in_sem.at[v])
        copy.start()
        loads.append(copy)
    tables = []
    for slot, (source, target) in enumerate(((ax_in, ax), (ay_in, ay), (az_in, az), (rx_in, rx),
                                             (ry_in, ry), (rz_in, rz), (ay_in, sy), (az_in, sz))):
        copy = pltpu.make_async_copy(source, target, table_sem.at[slot])
        copy.start()
        tables.append(copy)

    barrier = pltpu.get_barrier_semaphore()
    total = 0
    for axis, count, place in zip(AXES, counts, me):
        for k in range(1, count):
            pl.semaphore_signal(barrier, inc=1, device_id={axis: lax.rem(place + k, count)}, device_id_type=MESH)
            total += 1
    for copy in loads:
        copy.wait()
    pl.semaphore_wait(barrier, total)

    def ring(axis, slot, down_src, down_dst, up_src, up_dst):
        count, place = counts[axis], me[axis]
        lower = lax.rem(place + count - 1, count)
        upper = lax.rem(place + 1, count)
        down = pltpu.make_async_remote_copy(
            src_ref=down_src, dst_ref=down_dst, send_sem=halo_send.at[slot], recv_sem=halo_recv.at[slot],
            device_id={AXES[axis]: lower}, device_id_type=MESH)
        up = pltpu.make_async_remote_copy(
            src_ref=up_src, dst_ref=up_dst, send_sem=halo_send.at[slot + 1], recv_sem=halo_recv.at[slot + 1],
            device_id={AXES[axis]: upper}, device_id_type=MESH)
        down.start()
        up.start()
        return [down, up]

    def spread(axis, src, dst, send, recv):
        count, place = counts[axis], me[axis]
        copies = []
        for k in range(1, count):
            copy = pltpu.make_async_remote_copy(
                src_ref=src, dst_ref=dst, send_sem=send(k - 1), recv_sem=recv(k - 1),
                device_id={AXES[axis]: lax.rem(place + k, count)}, device_id_type=MESH)
            copy.start()
            copies.append(copy)
        return copies

    z_halo = ring(2, 4,
                  uz.at[:, pl.ds(2 * cy, 2 * cy)], uz.at[:, pl.ds((cz + 2) * cy, 2 * cy)],
                  uz.at[:, pl.ds(cz * cy, 2 * cy)], uz.at[:, pl.ds(0, 2 * cy)])

    sub8, lane8 = iota((8, cx), 0), iota((8, cx), 1)
    target = jnp.where(sub8 < 2, sub8, cx - 4 + sub8)
    select = jnp.where((sub8 < 4) & (lane8 == target), 1.0, 0.0).astype(jnp.float32)
    sub_h = iota((8, rows), 0)
    for group in range(0, nv, 4):
        low = jnp.zeros((8, rows), jnp.float32)
        high = low
        for v in range(group, min(group + 4, nv)):
            place = v - group
            ends = exact_dot(select, uz[v, pl.ds(2 * cy, rows), :], NT)
            mine = sub_h // 2 == place
            low = jnp.where(mine, pltpu.roll(ends, (2 * place) % 8, 0), low)
            high = jnp.where(mine, pltpu.roll(ends, (2 * place - 2) % 8, 0), high)
        hx[0, group // 4] = low
        hx[1, group // 4] = high
    x_halo = ring(0, 0, hx.at[0], hx.at[2], hx.at[1], hx.at[3])

    for v in range(nv):
        for y in range(cy):
            uy[v, pl.ds((y + 2) * cz, cz), :] = uz[v, pl.ds(2 * cy + y, cz, stride=cy), :]
    y_halo = ring(1, 2,
                  uy.at[:, pl.ds(2 * cz, 2 * cz)], uy.at[:, pl.ds((cy + 2) * cz, 2 * cz)],
                  uy.at[:, pl.ds(cy * cz, 2 * cz)], uy.at[:, pl.ds(0, 2 * cz)])

    for copy in tables[:4]:
        copy.wait()

    spread_z = jnp.where(iota((cz, rows), 1) // cy == iota((cz, rows), 0), 1.0, 0.0).astype(jnp.float32)
    spread_y = jnp.where(lax.rem(iota((cy, rows), 1), cy) == iota((cy, rows), 0), 1.0, 0.0).astype(jnp.float32)
    for v in range(nv):
        azx[...] = exact_dot(az[v], spread_z, NN)
        wide_y = exact_dot(ay[v], spread_y, NN)

        @pl.loop(0, cz)
        def _(z):
            high, low = halves(azx[pl.ds(z, 1), :] * wide_y)
            at = pl.ds(pl.multiple_of(z * cy, cy), cy)
            khi[v, at, :] = high
            klo[v, at, :] = low

    ux = []
    picked = iota((8 * gx, 4 * gx), 0)
    wanted = jnp.where(lax.rem(picked, 8) < 4, (picked // 8) * 4 + lax.rem(picked, 8), -1)
    expand = jnp.where(iota((8 * gx, 4 * gx), 1) == wanted, 1.0, 0.0).astype(jnp.float32)
    sub_m = iota((8, 4 * gx), 0)
    for v in range(nv):
        m = coupling(rx, me[0], gx, adv[0, v], lambda row: rx[v, pl.ds(row, 1), :])
        table = jnp.where(sub_m == 0, m[0], jnp.where(sub_m == 1, m[1], jnp.where(sub_m == 2, m[2],
                          jnp.where(sub_m == 3, m[3], 0.0))))
        columns = exact_dot(select, ax[v], NT)
        ux.append(exact_dot(exact_dot(expand, table, NT), columns, NN))

    def part(u, direction, centre_values=None):
        ahead = fluxes(u[1], direction)
        behind = fluxes(u[-1], direction)
        found = []
        for v in range(nv):
            fourth = u[-2][v] - 4.0 * u[-1][v] + 6.0 * u[0][v] - 4.0 * u[1][v] + u[2][v]
            found.append(-0.5 * (ahead[v] - behind[v]) - damping * fourth)
        return found

    for copy in y_halo:
        copy.wait_recv()

    @pl.loop(0, cy)
    def _(y):
        u = {}
        for off in range(-2, 3):
            at = pl.ds(pl.multiple_of((y + 2 + off) * cz, cz), cz)
            u[off] = [uy[v, at, :] for v in range(nv)]
        found = part(u, 1)
        for v in range(nv):
            res[v, pl.ds(y, cz, stride=cy), :] = found[v]

    for copy in x_halo:
        copy.wait_recv()
    merged = []
    for v in range(nv):
        fill = 1.0 if v == 0 else 0.0
        place = v % 4
        both = jnp.where(sub_h < 2, pltpu.roll(hx[2, v // 4], (-2 * place) % 8, 0),
                         pltpu.roll(hx[3, v // 4], (2 - 2 * place) % 8, 0))
        merged.append(jnp.where(sub_h < 4, both, fill))
    halo_flux = fluxes(merged, 0)

    def at_lane(row, lane, value):
        return jnp.where((sub8 == row) & (lane8 == lane), value, 0.0)

    weights = (at_lane(0, cx - 2, -damping) + at_lane(0, cx - 1, 4.0 * damping) + at_lane(1, cx - 1, -damping)
               + at_lane(2, 0, -damping) + at_lane(3, 0, 4.0 * damping) + at_lane(3, 1, -damping)
               + at_lane(4, cx - 1, -0.5) + at_lane(7, 0, 0.5)).astype(jnp.float32)
    for v in range(nv):
        stacked = jnp.where(sub_h < 4, merged[v], pltpu.roll(halo_flux[v], 4, 0))
        edge[v] = exact_dot(stacked, weights, TN)

    for copy in z_halo:
        copy.wait_recv()

    step = 2 * cy
    lane = iota((step, cx), 1)

    def shifted(a, offset):
        moved = pltpu.roll(a, (-offset) % cx, 1)
        inside = lane < cx - offset if offset > 0 else lane >= -offset
        return jnp.where(inside, moved, 0.0)

    def body(i, carry):
        squares, top = carry
        base = pl.multiple_of(i * step, step)
        u = {}
        for off in range(-2, 3):
            at = pl.ds(pl.multiple_of(base + (off + 2) * cy, cy), step)
            u[off] = [uz[v, at, :] for v in range(nv)]
        found = part(u, 2)
        values = primitives(u[0])
        velocity, internal, _ = values
        wave = (jnp.abs(velocity[0]) + jnp.abs(velocity[1]) + jnp.abs(velocity[2])
                + jnp.sqrt(3.0 * 1.4 * gas_ratio * internal))
        top = jnp.maximum(top, wave)
        flux_x = fluxes(u[0], 0, values)
        new_squares = []
        for v in range(nv):
            c = u[0][v]
            fourth = (shifted(c, -2) + shifted(c, 2)) - 4.0 * (shifted(c, -1) + shifted(c, 1)) + 6.0 * c
            along_x = -0.5 * (shifted(flux_x[v], 1) - shifted(flux_x[v], -1)) - damping * fourth
            at = pl.ds(base, step)
            value = res[v, at, :] + found[v] + (along_x + edge[v, at, :])
            res[v, at, :] = value
            new_squares.append(squares[v] + value * value)
        return tuple(new_squares), top

    zero = jnp.zeros((step, cx), jnp.float32)
    squares, top = lax.fori_loop(0, cz // 2, body, ((zero,) * nv, zero))

    x_copies = []
    for v in range(nv):
        parts = halves(res[v])
        across = halves(ax[v])
        xb[v, me[0]] = split_dot(halves(exact_dot(select, ax[v], NN)), parts, NT)
        x_copies.append(spread(0, xb.at[v, me[0]], xb.at[v, me[0]],
                               lambda k: xs.at[v, k], lambda k: xr.at[v, k]))
        first[v] = split_dot(parts, across, NT)

    sub_s = iota((8, cx), 0)
    tile = jnp.where(sub_s == 5, jnp.max(top, axis=0, keepdims=True), 0.0)
    for v in range(nv):
        tile = jnp.where(sub_s == v, jnp.sum(squares[v], axis=0, keepdims=True), tile)
    stx[me[0]] = tile
    stat_copies = [spread(0, stx.at[me[0]], stx.at[me[0]], lambda k: ss.at[0, k], lambda k: sr.at[0, k])]

    def gathered(ref, count):
        result = ref[0]
        for q in range(1, count):
            result = jnp.where(sub_s < nv, result + ref[q], jnp.maximum(result, ref[q]))
        return result

    y_copies = []
    marks_y = (0, 1, cy - 2, cy - 1)
    marks_z = (0, 1, cz - 2, cz - 1)
    for v in range(nv):
        for copy in x_copies[v]:
            copy.wait_recv()
        every = xb[v].reshape(8 * gx, rows)
        solved = first[v] - split_dot(halves(every), halves(ux[v]), TN)
        parts = halves(solved)
        field[v] = split_dot((khi[v], klo[v]), parts, NN)
        for c, mark in enumerate(marks_y):
            yb[v, me[1], pl.ds(c * cz, cz), :] = field[v, pl.ds(mark, cz, stride=cy), :]
        y_copies.append(spread(1, yb.at[v, me[1]], yb.at[v, me[1]],
                               lambda k: ys.at[v, k], lambda k: yr.at[v, k]))

    for copy in stat_copies[0]:
        copy.wait_recv()
    sty[me[1]] = gathered(stx, gx)
    stat_copies.append(spread(1, sty.at[me[1]], sty.at[me[1]], lambda k: ss.at[1, k], lambda k: sr.at[1, k]))

    def combined(reduced, inverse, axis, v, direction, planes, size):
        count = counts[axis]
        sums = [None] * 4
        for j in range(4 * count):
            m = coupling(reduced, me[axis], count, adv[direction, v], lambda row: reduced[v, row, j])
            plane = planes[v, j // 4, pl.ds((j % 4) * size, size), :]
            for c in range(4):
                term = m[c] * plane
                sums[c] = term if sums[c] is None else sums[c] + term
        return sums

    level, levels = me[2], gz
    low = jnp.maximum(4 * level - 2, 0)
    high = jnp.minimum(4 * level + 4, 4 * levels - 2)
    own = 4 * level
    has_low, has_high = level > 0, level < levels - 1
    z_copies = []
    for v in range(nv):
        up = pltpu.make_async_remote_copy(
            src_ref=zt.at[v, 0], dst_ref=zt.at[v, 2], send_sem=zs.at[v, 0], recv_sem=zr.at[v, 0],
            device_id={"gz": jnp.minimum(level + 1, levels - 1)}, device_id_type=MESH)
        down = pltpu.make_async_remote_copy(
            src_ref=zt.at[v, 1], dst_ref=zt.at[v, 3], send_sem=zs.at[v, 1], recv_sem=zr.at[v, 1],
            device_id={"gz": jnp.maximum(level - 1, 0)}, device_id_type=MESH)
        z_copies.append((up, down))

    def planes_of(v):
        return [field[v, pl.ds(mark * cy, cy), :] for mark in marks_z]

    def from_own(v, row, planes):
        return ((rz[v, row, own] * planes[0] + rz[v, row, own + 1] * planes[1])
                + (rz[v, row, own + 2] * planes[2] + rz[v, row, own + 3] * planes[3]))

    def carrier(v, corner, valid):
        x00, x01 = rz[v, corner, corner], rz[v, corner, corner + 1]
        x10, x11 = rz[v, corner + 1, corner], rz[v, corner + 1, corner + 1]
        inverse = 1.0 / jnp.full((cy, cx), jnp.where(valid, x00 * x11 - x01 * x10, 1.0), jnp.float32)

        def apply(row, pair):
            a, b = rz[v, row, corner], rz[v, row, corner + 1]
            return ((a * x11 - b * x10) * pair[0] + (b * x00 - a * x01) * pair[1]) * inverse

        return apply

    def pair_of(v, slot):
        return [zt[v, slot, pl.ds(0, cy), :], zt[v, slot, pl.ds(cy, cy), :]]

    for copy in tables[4:]:
        copy.wait()
    for v in range(nv):
        for copy in y_copies[v]:
            copy.wait_recv()
        sums = combined(ry, sy, 1, v, 1, yb, cz)
        for y in range(cy):
            at = pl.ds(y, cz, stride=cy)
            value = field[v, at, :]
            for c, mark in enumerate(marks_y):
                value = value - sy[v, y, mark] * sums[c]
            field[v, at, :] = value
        planes = planes_of(v)
        for r in range(2):
            zt[v, 0, pl.ds(r * cy, cy), :] = from_own(v, own + 2 + r, planes)
            zt[v, 1, pl.ds(r * cy, cy), :] = from_own(v, own + r, planes)

        @pl.when(level == 0)
        def _():
            zt[v, 2] = jnp.zeros((2 * cy, cx), jnp.float32)
            z_copies[v][0].start()

        @pl.when(level == levels - 1)
        def _():
            zt[v, 3] = jnp.zeros((2 * cy, cx), jnp.float32)
            z_copies[v][1].start()

        if v == 0:
            for copy in stat_copies[1]:
                copy.wait_recv()
            stz[me[2]] = gathered(sty, gy)
            stat_copies.append(spread(2, stz.at[me[2]], stz.at[me[2]],
                                      lambda k: ss.at[2, k], lambda k: sr.at[2, k]))

    def relay(v, way):
        copy = z_copies[v][way]
        corner, valid, row = ((low, has_low, own + 2), (high, has_high, own))[way]

        @pl.when(valid)
        def _():
            copy.wait_recv()

        @pl.when(has_low & has_high)
        def _():
            pair, apply = pair_of(v, 2 + way), carrier(v, corner, valid)
            for r in range(2):
                at = pl.ds(r * cy, cy)
                zt[v, way, at, :] = zt[v, way, at, :] + apply(row + r, pair)
            copy.start()

    def relay_all(ways):
        for way in ways:
            for v in range(nv):
                relay(v, way)

    @pl.when(2 * level < levels)
    def _():
        relay_all((0, 1))

    @pl.when(2 * level >= levels)
    def _():
        relay_all((1, 0))

    for copy in stat_copies[2]:
        copy.wait_recv()
    final = gathered(stz, gz)
    norm = jnp.sqrt(jnp.sum(final, axis=1, keepdims=True) / float(cells))
    norm = jnp.broadcast_to(norm, (8, cx))
    for v in range(nv):
        rms_out[v] = norm[v, 0]
    fastest = jnp.broadcast_to(courant / jnp.max(final, axis=1, keepdims=True), (8, cx))
    time_step = jnp.broadcast_to(fastest[5:6, :], (cy, cx))
    inner = jnp.where(has_low, 1.0, 0.0).astype(jnp.float32)
    outer = jnp.where(has_high, 1.0, 0.0).astype(jnp.float32)
    for v in range(nv):
        planes = planes_of(v)
        below, above = pair_of(v, 2), pair_of(v, 3)
        lift, sink = carrier(v, low, has_low), carrier(v, high, has_high)
        l = [inner * (below[r] + from_own(v, low + r, planes) + sink(low + r, above)) for r in range(2)]
        f = [outer * (above[r] + from_own(v, high + r, planes) + lift(high + r, below)) for r in range(2)]
        speed = adv[2, v]
        sums = [fourth_coef * l[0] + (-0.5 * speed - 4.0 * fourth_coef) * l[1],
                fourth_coef * l[1],
                fourth_coef * f[0],
                (0.5 * speed - 4.0 * fourth_coef) * f[0] + fourth_coef * f[1]]
        for z in range(cz):
            value = field[v, pl.ds(z * cy, cy), :]
            for c, mark in enumerate(marks_z):
                value = value - sz[v, z, mark] * sums[c]
            out[v, pl.ds(z * cy, cy), :] = value * time_step

    for group in [x_halo, y_halo, z_halo] + x_copies + y_copies + stat_copies:
        for copy in group:
            copy.wait_send()
    for v in range(nv):
        @pl.when(has_high)
        def _():
            z_copies[v][0].wait_send()

        @pl.when(has_low)
        def _():
            z_copies[v][1].wait_send()


def shards(counts, flow_state, advection, inverse_x, inverse_y, inverse_z, reduced_x, reduced_y, reduced_z):
    nv, cz, cy, cx = flow_state.shape
    gx, gy, gz = counts
    rows = cz * cy
    cells = rows * cx * gx * gy * gz
    most = max(counts) - 1
    vmem = pl.BlockSpec(memory_space=pltpu.VMEM)
    smem = pl.BlockSpec(memory_space=pltpu.SMEM)
    f32 = jnp.float32
    dma = pltpu.SemaphoreType.DMA
    hbm = pl.BlockSpec(memory_space=pl.ANY)
    out, rms = pl.pallas_call(
        functools.partial(kernel, (counts, nv, cz, cy, cx, cells)),
        out_shape=(jax.ShapeDtypeStruct((nv, rows, cx), f32), jax.ShapeDtypeStruct((nv,), f32)),
        in_specs=[hbm] * 7 + [smem],
        out_specs=(vmem, smem),
        scratch_shapes=[
            pltpu.VMEM(inverse_x.shape, f32),
            pltpu.VMEM(inverse_y.shape, f32),
            pltpu.VMEM(inverse_z.shape, f32),
            pltpu.VMEM(reduced_x.shape, f32),
            pltpu.SMEM(inverse_y.shape, f32),
            pltpu.SMEM(inverse_z.shape, f32),
            pltpu.SMEM(reduced_y.shape, f32),
            pltpu.SMEM(reduced_z.shape, f32),
            pltpu.VMEM((nv, (cz + 4) * cy, cx), f32),
            pltpu.VMEM((nv, (cy + 4) * cz, cx), f32),
            pltpu.VMEM((4, -(-nv // 4), 8, rows), f32),
            pltpu.VMEM((nv, rows, cx), f32),
            pltpu.VMEM((nv, rows, cx), f32),
            pltpu.VMEM((nv, rows, cx), f32),
            pltpu.VMEM((nv, rows, cx), f32),
            pltpu.VMEM((nv, gx, 8, rows), f32),
            pltpu.VMEM((nv, gy, 4 * cz, cx), f32),
            pltpu.VMEM((nv, 4, 2 * cy, cx), f32),
            pltpu.VMEM((gx, 8, cx), f32),
            pltpu.VMEM((gy, 8, cx), f32),
            pltpu.VMEM((gz, 8, cx), f32),
            pltpu.VMEM((nv, rows, rows), jnp.bfloat16),
            pltpu.VMEM((nv, rows, rows), jnp.bfloat16),
            pltpu.VMEM((cz, rows), f32),
            dma((nv,)), dma((8,)),
            dma((6,)), dma((6,)),
            dma((nv, gx - 1)), dma((nv, gx - 1)),
            dma((nv, gy - 1)), dma((nv, gy - 1)),
            dma((nv, 2)), dma((nv, 2)),
            dma((3, most)), dma((3, most)),
        ],
        compiler_params=pltpu.CompilerParams(
            collective_id=0, has_side_effects=True, vmem_limit_bytes=60 * 1024 * 1024),
    )(flow_state.reshape(nv, rows, cx), inverse_x, inverse_y, inverse_z, reduced_x, reduced_y, reduced_z,
      advection)
    return out.reshape(flow_state.shape), rms


def solution(mesh):
    counts = tuple(mesh.shape[axis] for axis in AXES)
    placed = (P(None, "gz", "gy", "gx"), P(), P(), P(), P(), P(), P(), P())
    return jax.shard_map(
        functools.partial(shards, counts),
        mesh=mesh,
        in_specs=placed,
        out_specs=(P(None, "gz", "gy", "gx"), P()),
        check_vma=False,
    )
```
